32 devices in a mesh: item: 4 (over z), var: 8 (over y, x, core).
Axes of the slice: x: 2, y: 2, z: 4, core: 2. Of those that a mesh axis runs over, the one named last changes fastest.
Arguments:
- pixels: bfloat16 [4, 64, 4, 2048], P('item', 'var'), may hold values from -6 to 6
- dataset: int32 [4], P('item'), may hold values from 0 to 4
- var_mask: int32 [5, 64], replicated, may hold values from 0 to 1, as said below
- data_weight: int32 [5], replicated, may hold values from 1 to 9
- emb_weight: bfloat16 [64, 4, 1024], P('var'), may hold values from -3 to 3
- var_embed: bfloat16 [64, 1024], P('var'), may hold values from -6 to 6
- agg_query: bfloat16 [1024], replicated, may hold values from -6 to 6
- agg_key: bfloat16 [1024, 1024], replicated, may hold values from -0.1875 to 0.1875
- agg_value: bfloat16 [1024, 1024], replicated, may hold values from -0.1875 to 0.1875
- agg_out: bfloat16 [1024, 1024], replicated, may hold values from -0.1875 to 0.1875
- ln1_gain: bfloat16 [1024], replicated, may hold values from 0.5 to 1.5
- ln1_bias: bfloat16 [1024], replicated, may hold values from -3 to 3
- qkv_weight: bfloat16 [1024, 3072], replicated, may hold values from -0.25 to 0.25
- proj_weight: bfloat16 [1024, 1024], replicated, may hold values from -0.75 to 0.75
- ln2_gain: bfloat16 [1024], replicated, may hold values from 0.5 to 1.5
- ln2_bias: bfloat16 [1024], replicated, may hold values from -3 to 3
- fc1_weight: bfloat16 [1024, 4096], replicated, may hold values from -0.1875 to 0.1875
- fc1_bias: bfloat16 [4096], replicated, may hold values from -3 to 3
- fc2_weight: bfloat16 [4096, 1024], replicated, may hold values from -0.09375 to 0.09375
- fc2_bias: bfloat16 [1024], replicated, may hold values from -3 to 3
- cotangent: bfloat16 [4, 2048, 1024], P('item', 'var'), may hold values from -6 to 6
Outputs:
- block_output: bfloat16 [4, 2048, 1024], P('item', 'var')
- pixels_grad: bfloat16 [4, 64, 4, 2048], P('item', 'var')
- emb_weight_grad: float32 [64, 4, 1024], P('var')
- var_embed_grad: float32 [64, 1024], P('var')
- agg_query_grad: float32 [1024], P('var')
- agg_key_grad: float32 [1024, 1024], P(None, 'var')
- agg_value_grad: float32 [1024, 1024], P(None, 'var')
- agg_out_grad: float32 [1024, 1024], P(None, 'var')
- ln1_gain_grad: float32 [1024], P('var')
- ln1_bias_grad: float32 [1024], P('var')
- qkv_weight_grad: float32 [1024, 3072], P(None, 'var')
- proj_weight_grad: float32 [1024, 1024], P(None, 'var')
- ln2_gain_grad: float32 [1024], P('var')
- ln2_bias_grad: float32 [1024], P('var')
- fc1_weight_grad: float32 [1024, 4096], P(None, 'var')
- fc1_bias_grad: float32 [4096], P('var')
- fc2_weight_grad: float32 [4096, 1024], P(None, 'var')
- fc2_bias_grad: float32 [1024], P('var')
The draws below stay inside these ranges and needn't reach their ends.
Inputs may be any that keep to these rules, and one draw needn't show every extreme that they name: `var_mask`: each dataset's list names at least one variable; no list names a slot whose index is 3 mod 4.
All inputs are finite; a program needn't handle non-finite values.
Results may differ from the reference program's by a relative error of at most 0.025.
Values may be sent and summed in bfloat16 or wider, within the bound.
A program may use at most 512 MiB of HBM per device.

```python
import jax
import jax.numpy as jnp
from jax import lax

D = 1024
HEADS = 16
HEAD_DIM = 64
FF = 4096
VARS = 64
PIX = 4
PATCHES = 2048
NDATA = 5
ITEMS = 4


def draw_var_mask(key, part):
    kept_slots = jax.random.randint(jax.random.fold_in(key, 11), (NDATA, VARS), 0, 4) != 0
    slot_index = jnp.arange(VARS, dtype=jnp.int32)
    real_slots = slot_index % 4 != 3
    forced = jax.random.randint(jax.random.fold_in(key, 12), (NDATA, 1), 0, VARS // 4) * 4
    listed = jnp.logical_or(jnp.logical_and(kept_slots, real_slots[None, :]), slot_index[None, :] == forced)
    return listed.astype(jnp.int32)


def with_ends(entries, stream_key, least, top_value):
    place = [jax.random.randint(jax.random.fold_in(stream_key, axis), (), 0, length) for axis, length in enumerate(entries.shape)]
    main_axis = entries.shape.index(max(entries.shape))
    beside = place[:main_axis] + [(place[main_axis] + 1) % entries.shape[main_axis]] + place[main_axis + 1:]
    return entries.at[tuple(place)].set(least).at[tuple(beside)].set(top_value)


def raised(array, stream_key, source, target, parts, factor):
    def block_of(dim):
        return (jnp.arange(array.shape[dim]) // (array.shape[dim] // parts)).reshape((-1,) + (1,) * (array.ndim - 1 - dim))

    first = jax.random.permutation(stream_key, parts)[block_of(target)]
    second = (block_of(target) + parts // 2) % parts
    return jnp.where((block_of(source) == first) | (block_of(source) == second), factor * array, array)


def steps_of(own_key, dims, split, smallest, largest):
    loudness = 1.0
    for position, parts in split:
        draws = jax.random.uniform(jax.random.fold_in(jax.random.fold_in(own_key, 6), position), (parts,), jnp.float32, smallest / len(split), largest / len(split))
        loudness = loudness * jnp.repeat(jnp.exp(draws), dims[position] // parts).reshape((-1,) + (1,) * (len(dims) - 1 - position))
    return loudness


def centred(stream_key, dims, width, most, cuts=(), held_as=jnp.bfloat16):
    gain = steps_of(stream_key, dims, cuts, -0.22, 0.18) if cuts else 1.0
    entries = jax.random.normal(stream_key, dims, jnp.float32) * width * gain
    return jnp.minimum(jnp.maximum(entries, -most), most).astype(held_as)


def noise_with(own_key, dims, deviation, bound, cuts, heavy, kind=jnp.bfloat16):
    entries = deviation * jax.random.normal(own_key, dims, jnp.float32)
    if cuts:
        entries = entries * steps_of(own_key, dims, cuts, -0.22, 0.18)
    return jnp.clip(raised(entries, jax.random.fold_in(own_key, 3), *heavy), -bound, bound).astype(kind)


def setup_inputs(seed: int = 0) -> dict:
    seeds = jax.random.split(jax.random.key(seed), 22)
    return {
        "pixels": centred(seeds[0], (ITEMS, VARS, PIX, PATCHES), 1.0, 6.0, ((0, 4), (1, 8))),
        "dataset": with_ends(jax.random.randint(seeds[1], (ITEMS,), 0, NDATA), jax.random.fold_in(seeds[1], 1), 0, NDATA - 1).astype(jnp.int32),
        "var_mask": draw_var_mask(jax.random.fold_in(seeds[21], 71), 0),
        "data_weight": with_ends(jax.random.randint(seeds[3], (NDATA,), 1, 10), jax.random.fold_in(seeds[3], 1), 1, 9).astype(jnp.int32),
        "emb_weight": centred(seeds[4], (VARS, PIX, D), PIX ** -0.5, 3.0, ((0, 8),)),
        "var_embed": centred(seeds[5], (VARS, D), 1.0, 6.0, ((0, 8),)),
        "agg_query": centred(seeds[6], (D,), 1.0, 6.0),
        "agg_key": centred(seeds[7], (D, D), D ** -0.5, 0.1875),
        "agg_value": centred(seeds[8], (D, D), D ** -0.5, 0.1875),
        "agg_out": centred(seeds[9], (D, D), D ** -0.5, 0.1875),
        "ln1_gain": jnp.clip(1.0 + 0.1 * jax.random.normal(seeds[10], (D,), jnp.float32), 0.5, 1.5).astype(jnp.bfloat16),
        "ln1_bias": centred(seeds[11], (D,), 0.5, 3.0),
        "qkv_weight": centred(seeds[12], (D, 3 * D), (D // 2) ** -0.5, 0.25),
        "proj_weight": centred(seeds[13], (D, D), HEAD_DIM ** -0.5, 0.75),
        "ln2_gain": jnp.clip(1.0 + 0.1 * jax.random.normal(seeds[14], (D,), jnp.float32), 0.5, 1.5).astype(jnp.bfloat16),
        "ln2_bias": centred(seeds[15], (D,), 0.5, 3.0),
        "fc1_weight": centred(seeds[16], (D, FF), D ** -0.5, 0.1875),
        "fc1_bias": centred(seeds[17], (FF,), 0.5, 3.0),
        "fc2_weight": centred(seeds[18], (FF, D), FF ** -0.5, 0.09375),
        "fc2_bias": centred(seeds[19], (D,), 0.5, 3.0),
        "cotangent": noise_with(seeds[20], (ITEMS, PATCHES, D), 1.0, 6.0, ((0, 4), (1, 8)), (1, 2, 8, 2.0)),
    }


@jax.custom_vjp
def low(v):
    return lax.optimization_barrier(v.astype(jnp.bfloat16)).astype(jnp.float32)

@jax.custom_vjp
def low_back(v):
    return v

def low_keep(v):
    return (low(v), None)

def low_pass(kept, grad):
    return (grad,)

def back_keep(v):
    return (v, None)

def back_low(kept, grad):
    return (low(grad),)
low.defvjp(low_keep, low_pass)
low_back.defvjp(back_keep, back_low)
PRECISE = lax.Precision.HIGHEST

def layer_norm(values, gain_vec, shift_vec):
    center = values - lax.optimization_barrier(jnp.mean(values, axis=-1, keepdims=True))
    spread = lax.optimization_barrier(jnp.mean(center * center, axis=-1, keepdims=True))
    return center * lax.rsqrt(spread + 1e-06) * gain_vec + shift_vec

def item_forward(params, pixel_item, live_item):
    emb_weight, var_embed, agg_query, agg_key, agg_value, agg_out, ln1_gain, ln1_bias, qkv_weight, proj_weight, ln2_gain, ln2_bias, fc1_weight, fc1_bias, fc2_weight, fc2_bias = params
    factor = HEAD_DIM ** (-0.5)
    tokens = jnp.einsum('vcp,vcd->vpd', pixel_item, emb_weight, precision=PRECISE) + var_embed[:, None, :]
    tokens = low_back(low(tokens))
    head_probe = low((agg_key * agg_query[None, :]).reshape(D, HEADS, HEAD_DIM).sum(axis=-1).T)
    agg_scores = low_back(jnp.einsum('vpd,hd->vph', tokens, head_probe, precision=PRECISE) * factor)
    present = live_item[:, None, None] > 0.5
    masked = jnp.where(present, agg_scores, -1e+30)
    highest = lax.optimization_barrier(jnp.max(masked, axis=0, keepdims=True))
    exp_terms = jnp.exp(masked - highest) * live_item[:, None, None]
    weights = low(exp_terms / lax.optimization_barrier(jnp.sum(exp_terms, axis=0, keepdims=True)))
    context = low_back(low(jnp.einsum('vph,vpd->phd', weights, tokens, precision=PRECISE)))
    agg_mixed = jnp.einsum('phd,dhe->phe', context, agg_value.reshape(D, HEADS, HEAD_DIM), precision=PRECISE)
    agg_mixed = low_back(low(agg_mixed.reshape(PATCHES, D)))
    agg_result = low_back(jnp.dot(agg_mixed, agg_out, precision=PRECISE))
    first_norm = low(layer_norm(agg_result, ln1_gain, ln1_bias))
    qkv_proj = low_back(low(jnp.dot(first_norm, qkv_weight, precision=PRECISE)))
    qkv_proj = qkv_proj.reshape(PATCHES, 3, HEADS, HEAD_DIM)
    scores = low_back(jnp.einsum('qhe,khe->hqk', qkv_proj[:, 0], qkv_proj[:, 1], precision=PRECISE) * factor)
    top_score = lax.optimization_barrier(jnp.max(scores, axis=-1, keepdims=True))
    score_terms = jnp.exp(scores - top_score)
    attn_probs = low(score_terms / lax.optimization_barrier(jnp.sum(score_terms, axis=-1, keepdims=True)))
    attended = jnp.einsum('hqk,khe->qhe', attn_probs, qkv_proj[:, 2], precision=PRECISE)
    attended = low_back(low(attended.reshape(PATCHES, D)))
    residual = agg_result + low_back(jnp.dot(attended, proj_weight, precision=PRECISE))
    second_norm = low(layer_norm(residual, ln2_gain, ln2_bias))
    pre_act = low_back(jnp.dot(second_norm, fc1_weight, precision=PRECISE) + fc1_bias)
    gelu_out = low(jax.nn.gelu(pre_act, approximate=False))
    return residual + low_back(jnp.dot(gelu_out, fc2_weight, precision=PRECISE) + fc2_bias)

def reference(pixels, dataset, var_mask, data_weight, emb_weight, var_embed, agg_query, agg_key, agg_value, agg_out, ln1_gain, ln1_bias, qkv_weight, proj_weight, ln2_gain, ln2_bias, fc1_weight, fc1_bias, fc2_weight, fc2_bias, cotangent):
    params = tuple((weight.astype(jnp.float32) for weight in (emb_weight, var_embed, agg_query, agg_key, agg_value, agg_out, ln1_gain, ln1_bias, qkv_weight, proj_weight, ln2_gain, ln2_bias, fc1_weight, fc1_bias, fc2_weight, fc2_bias)))
    live_mask = var_mask[dataset].astype(jnp.float32)
    counts = data_weight.astype(jnp.float32)
    item_scale = counts[dataset] * NDATA / jnp.sum(counts)

    def forward(pixel_all, weight_set):

        def one_item(item_pair):
            return item_forward(weight_set, item_pair[0], item_pair[1])
        return lax.map(jax.checkpoint(one_item), (pixel_all, live_mask))
    block_out, pullback = jax.vjp(forward, pixels.astype(jnp.float32), params)
    grad_out = cotangent.astype(jnp.float32) * item_scale[:, None, None]
    pixel_grad, weight_grads = pullback(grad_out)
    g_emb, g_var, g_query, g_key, g_value, g_out, g_ln1_gain, g_ln1_bias, g_qkv, g_proj, g_ln2_gain, g_ln2_bias, g_fc1, g_fc1_bias, g_fc2, g_fc2_bias = weight_grads
    return (block_out.astype(jnp.bfloat16), pixel_grad.astype(jnp.bfloat16), g_emb, g_var, g_query, g_key, g_value, g_out, g_ln1_gain, g_ln1_bias, g_qkv, g_proj, g_ln2_gain, g_ln2_bias, g_fc1, g_fc1_bias, g_fc2, g_fc2_bias)
```

```python
import jax
import jax.numpy as jnp
from jax import lax
from jax.sharding import PartitionSpec as P

D = 1024
HEADS = 16
HEAD_DIM = 64
PATCHES = 2048
NDATA = 5
PRECISE = lax.Precision.HIGHEST
FACTOR = HEAD_DIM ** (-0.5)
F32 = jnp.float32
BF16 = jnp.bfloat16


def mm(spec, a, b):
    return jnp.einsum(spec, a, b, preferred_element_type=F32)


def norm_stats(values):
    center = values - jnp.mean(values, axis=-1, keepdims=True)
    spread = jnp.mean(center * center, axis=-1, keepdims=True)
    inv = lax.rsqrt(spread + 1e-06)
    return center * inv, inv


def norm_back(grad, gain_vec, normed, inv):
    u = grad * gain_vec
    mean_u = jnp.mean(u, axis=-1, keepdims=True)
    mean_un = jnp.mean(u * normed, axis=-1, keepdims=True)
    return inv * (u - mean_u - normed * mean_un)


def listed(array, axis):
    shape = array.shape
    split = shape[:axis] + (shape[axis] // 4, 4) + shape[axis + 1 :]
    kept = lax.slice_in_dim(array.reshape(split), 0, 3, axis=axis + 1)
    return kept.reshape(shape[:axis] + (shape[axis] // 4 * 3,) + shape[axis + 1 :])


def unlisted(array, axis):
    shape = array.shape
    split = shape[:axis] + (shape[axis] // 3, 3) + shape[axis + 1 :]
    pads = [(0, 0)] * len(split)
    pads[axis + 1] = (0, 1)
    full = jnp.pad(array.reshape(split), pads)
    return full.reshape(shape[:axis] + (shape[axis] // 3 * 4,) + shape[axis + 1 :])


def to_heads(rows, lanes, parts):
    g, r, _ = rows.shape
    wide = rows.reshape(g, r, parts, lanes, D // lanes)
    out = lax.all_to_all(wide, "var", split_axis=3, concat_axis=1, tiled=True)
    return out.reshape(g, r * lanes, parts, D // lanes)


def from_heads(cols, lanes):
    g, p, parts, w = cols.shape
    out = lax.all_to_all(
        cols.reshape(g, p, parts, 1, w), "var", split_axis=1, concat_axis=3, tiled=True
    )
    return out.reshape(g, p // lanes, parts * w * lanes)


def attention_forward(queries, keys, values):
    scores = mm("gshe,gkhe->ghsk", queries, keys) * FACTOR
    highest = jnp.max(scores, axis=-1, keepdims=True)
    terms = jnp.exp(scores - highest)
    totals = jnp.sum(terms, axis=-1, keepdims=True)
    attended = mm("ghsk,gkhe->gshe", (terms / totals).astype(BF16), values)
    return attended, highest + jnp.log(totals)


def attention_back(queries, keys, values, g_att, lse, rowdot):
    probs = jnp.exp(mm("gshe,gkhe->ghsk", queries, keys) * FACTOR - lse)
    g_probs = mm("gshe,gkhe->ghsk", g_att, values)
    g_scores = (probs * (g_probs - rowdot)).astype(BF16)
    g_q = mm("ghsk,gkhe->gshe", g_scores, keys) * FACTOR
    g_k = mm("ghsk,gshe->gkhe", g_scores, queries) * FACTOR
    g_v = mm("ghsk,gshe->gkhe", probs.astype(BF16), g_att)
    return g_q, g_k, g_v


def body(
    pixels,
    dataset,
    var_mask,
    data_weight,
    emb_weight,
    var_embed,
    agg_query,
    agg_key,
    agg_value,
    agg_out,
    ln1_gain,
    ln1_bias,
    qkv_weight,
    proj_weight,
    ln2_gain,
    ln2_bias,
    fc1_weight,
    fc1_bias,
    fc2_weight,
    fc2_bias,
    cotangent,
):
    g = pixels.shape[0]
    slots = var_mask.shape[1]
    pix = pixels.shape[2]
    lanes = lax.axis_size("var")
    own_slots = slots // lanes
    mine = lax.axis_index("var")
    r = PATCHES // lanes
    rows = g * r
    live = slots // 4 * 3
    hot = (dataset[:, None] == jnp.arange(NDATA, dtype=jnp.int32)[None, :]).astype(F32)
    counts = data_weight.astype(F32)
    item_scale = jnp.dot(hot, counts, precision=PRECISE) * NDATA / jnp.sum(counts)
    mask = listed(jnp.dot(hot, var_mask.astype(F32), precision=PRECISE), 1)

    own_table = jnp.concatenate([emb_weight, var_embed[:, None, :]], axis=1)
    table = lax.all_gather(own_table, "var", axis=0, tiled=True)
    table = jnp.transpose(listed(table, 0), (1, 0, 2))
    flat_table = table.reshape((pix + 1) * live, D)
    patch_pix = lax.all_to_all(pixels, "var", split_axis=3, concat_axis=1, tiled=True)
    patch_pix = jnp.transpose(listed(patch_pix, 1), (0, 2, 1, 3))
    xs = jnp.concatenate([patch_pix, jnp.ones((g, 1, live, r), BF16)], axis=1)

    query_full = agg_query.astype(F32)
    key_full = agg_key.astype(F32)
    probe = (key_full * query_full[None, :]).reshape(D, HEADS, HEAD_DIM).sum(axis=-1)
    probe = probe.T.astype(BF16)
    seen = mm("xd,hd->hx", flat_table, probe).reshape(HEADS, pix + 1, live) * FACTOR
    ev = mm("xd,de->xe", flat_table, agg_value).astype(BF16)
    ev_heads = ev.reshape(pix + 1, live, HEADS, HEAD_DIM)

    xf = xs.astype(F32)
    scores = sum(seen[None, :, c, :, None] * xf[:, None, c] for c in range(pix + 1))
    present = mask[:, None, :, None]
    scores = jnp.where(present > 0.5, scores, -1e30)
    highest = jnp.max(scores, axis=2, keepdims=True)
    terms = jnp.exp(scores - highest) * present
    weights = terms / jnp.sum(terms, axis=2, keepdims=True)
    low = weights.astype(BF16)
    wx = low[:, :, None] * xs[:, None]
    mixed = mm("ghcvr,cvhe->grhe", wx, ev_heads).astype(BF16).reshape(rows, D)
    result = jnp.dot(mixed, agg_out, preferred_element_type=F32)

    vectors = [v.astype(F32) for v in (ln1_gain, ln1_bias, ln2_gain, ln2_bias, fc1_bias, fc2_bias)]
    gain1, shift1, gain2, shift2, bias1, bias2 = vectors
    normed1, inv1 = norm_stats(result)
    first = (normed1 * gain1 + shift1).astype(BF16)
    qkv = jnp.dot(first, qkv_weight, preferred_element_type=F32).astype(BF16).reshape(g, r, 3 * D)

    by_head = HEADS % lanes == 0
    if by_head:
        own_heads = HEADS // lanes
        heads = to_heads(qkv, lanes, 3).reshape(g, PATCHES, 3, own_heads, HEAD_DIM)
        queries, keys, values = heads[:, :, 0], heads[:, :, 1], heads[:, :, 2]
    else:
        queries = qkv[..., :D].reshape(g, r, HEADS, HEAD_DIM)
        pair = lax.all_gather(qkv[..., D:], "var", axis=1, tiled=True)
        pair = pair.reshape(g, PATCHES, 2, HEADS, HEAD_DIM)
        keys, values = pair[:, :, 0], pair[:, :, 1]
    att_full, lse = attention_forward(queries, keys, values)
    att = att_full.astype(BF16).reshape(g, att_full.shape[1], -1)
    if by_head:
        attended = from_heads(att[:, :, None, :], lanes).reshape(rows, D)
    else:
        attended = att.reshape(rows, D)

    residual = result + jnp.dot(attended, proj_weight, preferred_element_type=F32)
    normed2, inv2 = norm_stats(residual)
    second = (normed2 * gain2 + shift2).astype(BF16)
    pre = jnp.dot(second, fc1_weight, preferred_element_type=F32) + bias1
    cdf = 0.5 * (1.0 + lax.erf(pre * (0.5**0.5)))
    slope = cdf + pre * jnp.exp(-0.5 * pre * pre) * 0.3989422804014327
    act = (pre * cdf).astype(BF16)
    block_out = residual + jnp.dot(act, fc2_weight, preferred_element_type=F32) + bias2

    g_final = (cotangent.astype(F32) * item_scale[:, None, None]).reshape(rows, D)
    g_mlp = g_final.astype(BF16)
    fc2_t = mm("rd,rf->df", g_mlp, act).astype(BF16)
    g_pre = (mm("rd,fd->rf", g_mlp, fc2_weight) * slope).astype(BF16)
    fc1_t = mm("rf,rd->fd", g_pre, second).astype(BF16)
    g_second = mm("rf,df->rd", g_pre, fc1_weight)
    g_resid = g_final + norm_back(g_second, gain2, normed2, inv2)
    g_branch = g_resid.astype(BF16)
    proj_t = mm("re,rd->ed", g_branch, attended).astype(BF16)
    g_att = mm("re,de->rd", g_branch, proj_weight).astype(BF16).reshape(g, r, D)
    if by_head:
        g_att = to_heads(g_att, lanes, 1)
    g_att = g_att.reshape(att_full.shape)
    rowdot = jnp.transpose(jnp.sum(g_att.astype(F32) * att_full, axis=-1), (0, 2, 1))[..., None]
    g_q, g_k, g_v = attention_back(queries, keys, values, g_att, lse, rowdot)
    if by_head:
        width = D // lanes
        parts = [t.astype(BF16).reshape(g, PATCHES, 1, width) for t in (g_q, g_k, g_v)]
        g_qkv = from_heads(jnp.concatenate(parts, axis=2), lanes)
    else:
        parts = [
            lax.psum_scatter(t, "var", scatter_dimension=1, tiled=True).reshape(g, r, D)
            for t in (g_k, g_v)
        ]
        g_qkv = jnp.concatenate([g_q.reshape(g, r, D)] + parts, axis=-1).astype(BF16)
    g_qkv = g_qkv.reshape(rows, 3 * D)
    qkv_t = mm("re,rd->ed", g_qkv, first).astype(BF16)
    g_first = mm("re,de->rd", g_qkv, qkv_weight)
    g_result = (g_resid + norm_back(g_first, gain1, normed1, inv1)).astype(BF16)
    out_t = mm("rd,rj->dj", g_result, mixed).astype(BF16)
    g_mixed = mm("rd,jd->rj", g_result, agg_out).astype(BF16).reshape(g, r, HEADS, HEAD_DIM)

    back = mm("cvhe,grhe->ghcvr", ev_heads, g_mixed)
    g_w = jnp.sum(back * xf[:, None], axis=2)
    rowsum = jnp.sum(weights * g_w, axis=2, keepdims=True)
    g_s = weights * (g_w - rowsum)
    pixel_grads = jnp.sum(low.astype(F32)[:, :, None] * back[:, :, :pix], axis=1)
    pixel_grads = pixel_grads + jnp.sum(
        g_s[:, :, None] * seen[None, :, :pix, :, None], axis=1
    )
    pixel_grads = unlisted(jnp.transpose(pixel_grads, (0, 2, 1, 3)).astype(BF16), 1)
    pixel_out = lax.all_to_all(pixel_grads, "var", split_axis=1, concat_axis=3, tiled=True)
    t_part = jnp.sum(g_s[:, :, None] * xf[:, None], axis=(0, 4))
    m_part = mm("ghcvr,grhe->cvhe", wx, g_mixed).reshape((pix + 1) * live, D)

    small = [
        jnp.sum(g_second * normed2, axis=0),
        jnp.sum(g_second, axis=0),
        jnp.sum(g_first * normed1, axis=0),
        jnp.sum(g_first, axis=0),
        jnp.sum(g_mlp.astype(F32), axis=0),
        jnp.sum(g_pre.astype(F32), axis=0),
        t_part.reshape(-1),
    ]
    sizes = [s.shape[0] for s in small]
    small_sum, m_sum = lax.psum((jnp.concatenate(small), m_part), ("item", "var"))
    ends = [sum(sizes[:k]) for k in range(len(sizes) + 1)]
    pieces = [small_sum[ends[k] : ends[k + 1]] for k in range(len(sizes))]

    def own(vector):
        width = vector.shape[0] // lanes
        return lax.dynamic_slice_in_dim(vector, mine * width, width)

    ln2_gain_grad, ln2_bias_grad, ln1_gain_grad, ln1_bias_grad, fc2_bias_grad, fc1_bias_grad = [
        own(p) for p in pieces[:6]
    ]
    t_sum = pieces[6].reshape(HEADS, (pix + 1) * live)

    m_slots = unlisted(m_sum.reshape(pix + 1, live, D), 1)
    t_slots = unlisted(t_sum.reshape(HEADS, pix + 1, live), 2)
    m_own = lax.dynamic_slice_in_dim(m_slots, mine * own_slots, own_slots, axis=1)
    t_own = lax.dynamic_slice_in_dim(t_slots, mine * own_slots, own_slots, axis=2)
    table_grad = mm("cve,de->vcd", m_own.astype(BF16), agg_value)
    table_grad = table_grad + jnp.einsum(
        "hcv,hd->vcd", t_own * FACTOR, probe.astype(F32), precision=PRECISE
    )
    width = D // lanes
    m_cols = lax.dynamic_slice_in_dim(m_sum, mine * width, width, axis=1)
    value_grad = mm("xd,xe->de", flat_table, m_cols.astype(BF16))
    g_probe = jnp.dot(t_sum, flat_table.astype(F32), precision=PRECISE) * FACTOR
    head_of = jnp.arange(D) // HEAD_DIM
    own_head = lax.dynamic_slice_in_dim(head_of, mine * width, width)
    pick = (own_head[None, :] == jnp.arange(HEADS)[:, None]).astype(F32)
    g_cols = jnp.einsum("hk,he->ke", g_probe, pick, precision=PRECISE)
    own_query = lax.dynamic_slice_in_dim(query_full, mine * width, width)
    own_key = lax.dynamic_slice_in_dim(agg_key, mine * width, width, axis=1).astype(F32)
    key_grad = g_cols * own_query[None, :]
    query_grad = jnp.sum(g_cols * own_key, axis=0)

    def reduced(grad):
        share = lax.psum_scatter(grad, "var", scatter_dimension=0, tiled=True)
        return lax.psum(share, "item").astype(F32).T

    fc2_grad, fc1_grad, proj_grad, qkv_grad, out_grad = [
        reduced(t) for t in (fc2_t, fc1_t, proj_t, qkv_t, out_t)
    ]
    return (
        block_out.reshape(g, r, D).astype(BF16),
        pixel_out,
        table_grad[:, :pix],
        table_grad[:, pix],
        query_grad,
        key_grad,
        value_grad,
        out_grad,
        ln1_gain_grad,
        ln1_bias_grad,
        qkv_grad,
        proj_grad,
        ln2_gain_grad,
        ln2_bias_grad,
        fc1_grad,
        fc1_bias_grad,
        fc2_grad,
        fc2_bias_grad,
    )


def solution(mesh):
    in_specs = (
        P("item", "var", None, None),
        P("item"),
        P(),
        P(),
        P("var", None, None),
        P("var", None),
        *([P()] * 14),
        P("item", "var", None),
    )
    cols = P(None, "var")
    vec = P("var")
    out_specs = (
        P("item", "var", None),
        P("item", "var", None, None),
        P("var", None, None),
        P("var", None),
        vec,
        cols,
        cols,
        cols,
        vec,
        vec,
        cols,
        cols,
        vec,
        vec,
        cols,
        vec,
        cols,
        vec,
    )
    return jax.shard_map(body, mesh=mesh, in_specs=in_specs, out_specs=out_specs, check_vma=False)
```

```python
import functools

import jax
import jax.numpy as jnp
from jax import lax
from jax.experimental import pallas as pl
from jax.experimental.pallas import tpu as pltpu
from jax.sharding import PartitionSpec as P

D = 1024
HEADS = 16
HEAD_DIM = 64
PATCHES = 2048
NDATA = 5
PRECISE = lax.Precision.HIGHEST
FACTOR = HEAD_DIM ** (-0.5)
F32 = jnp.float32
BF16 = jnp.bfloat16
MESH = pl.DeviceIdType.MESH
KEY_PARTS = 4


def mm(spec, a, b):
    return jnp.einsum(spec, a, b, preferred_element_type=F32)


def norm_stats(values):
    center = values - jnp.mean(values, axis=-1, keepdims=True)
    spread = jnp.mean(center * center, axis=-1, keepdims=True)
    inv = lax.rsqrt(spread + 1e-06)
    return center * inv, inv


def norm_back(grad, gain_vec, normed, inv):
    u = grad * gain_vec
    mean_u = jnp.mean(u, axis=-1, keepdims=True)
    mean_un = jnp.mean(u * normed, axis=-1, keepdims=True)
    return inv * (u - mean_u - normed * mean_un)


def listed(array, axis):
    shape = array.shape
    split = shape[:axis] + (shape[axis] // 4, 4) + shape[axis + 1 :]
    kept = lax.slice_in_dim(array.reshape(split), 0, 3, axis=axis + 1)
    return kept.reshape(shape[:axis] + (shape[axis] // 4 * 3,) + shape[axis + 1 :])


def unlisted(array, axis):
    shape = array.shape
    split = shape[:axis] + (shape[axis] // 3, 3) + shape[axis + 1 :]
    pads = [(0, 0)] * len(split)
    pads[axis + 1] = (0, 1)
    full = jnp.pad(array.reshape(split), pads)
    return full.reshape(shape[:axis] + (shape[axis] // 3 * 4,) + shape[axis + 1 :])


def attention_forward(queries, keys, values):
    scores = mm("gshe,gkhe->ghsk", queries, keys) * FACTOR
    highest = jnp.max(scores, axis=-1, keepdims=True)
    terms = jnp.exp(scores - highest)
    totals = jnp.sum(terms, axis=-1, keepdims=True)
    attended = mm("ghsk,gkhe->gshe", (terms / totals).astype(BF16), values)
    return attended, highest + jnp.log(totals)


def attention_back(queries, keys, values, g_att, lse, rowdot):
    probs = jnp.exp(mm("gshe,gkhe->ghsk", queries, keys) * FACTOR - lse)
    g_probs = mm("gshe,gkhe->ghsk", g_att, values)
    g_scores = (probs * (g_probs - rowdot)).astype(BF16)
    g_q = mm("ghsk,gkhe->gshe", g_scores, keys) * FACTOR
    g_k = mm("ghsk,gshe->gkhe", g_scores, queries) * FACTOR
    g_v = mm("ghsk,gshe->gkhe", probs.astype(BF16), g_att)
    return g_q, g_k, g_v


def greet(me, n):
    barrier = pltpu.get_barrier_semaphore()
    for i in range(1, n):
        pl.semaphore_signal(
            barrier, inc=1, device_id={"var": lax.rem(me + i, n)}, device_id_type=MESH
        )
    pl.semaphore_wait(barrier, n - 1)


def nt(a, b):
    return lax.dot_general(a, b, (((1,), (1,)), ((), ())), preferred_element_type=F32)


def nn(a, b):
    return jnp.dot(a, b, preferred_element_type=F32)


def head_masks(width):
    lane = lax.broadcasted_iota(jnp.int32, (1, width), 1) // HEAD_DIM
    return [(lane == h).astype(F32) for h in range(width // HEAD_DIM)]


def forward_kernel(
    n, qkv, heads, o_out, lse_out, att_out, recv, land, obuf, v_t, s_buf,
    send, got, back_send, back_got, out_sem,
):
    me = lax.axis_index("var")
    rows, total = qkv.shape
    dim = total // 3
    width = dim // n
    patches = rows * n
    mine = pl.ds(pl.multiple_of(me * rows, rows), rows)
    own_lanes = pl.ds(pl.multiple_of(me * width, width), width)
    greet(me, n)

    def out_copy(s, i):
        to = lax.rem(me + i, n)
        return pltpu.make_async_remote_copy(
            src_ref=qkv.at[:, pl.ds(pl.multiple_of(s * dim + to * width, width), width)],
            dst_ref=recv.at[s, mine, :],
            send_sem=send.at[s, i],
            recv_sem=got.at[s, i],
            device_id={"var": to},
            device_id_type=MESH,
        )

    def back_copy(i):
        to = lax.rem(me - i + n, n)
        return pltpu.make_async_remote_copy(
            src_ref=obuf.at[i],
            dst_ref=land.at[:, own_lanes],
            send_sem=back_send.at[i],
            recv_sem=back_got.at[i],
            device_id={"var": to},
            device_id_type=MESH,
        )

    for s in (1, 2, 0):
        for i in range(1, n):
            out_copy(s, i).start()
    for s in (1, 2, 0):
        recv[s, mine, :] = qkv[:, pl.ds(pl.multiple_of(s * dim + me * width, width), width)]
    masks = head_masks(width)
    for s in (1, 2):
        for i in range(1, n):
            out_copy(s, i).wait_recv()
    v_t[...] = recv[2].T
    chunk = s_buf.shape[0] // KEY_PARTS

    def block(i, carry):
        source = lax.rem(me - i + n, n)

        @pl.when(i > 0)
        def _():
            out_copy(0, i).wait_recv()

        place = pl.ds(pl.multiple_of(source * rows, rows), rows)
        q = recv[0, place, :].astype(F32) * FACTOR
        outs = []
        for h, mask in enumerate(masks):
            qh = (q * mask).astype(BF16)
            high = None
            for c in range(KEY_PARTS):
                part = slice(c * chunk, (c + 1) * chunk)
                scores = nt(recv[1, part, :], qh)
                s_buf[part, :] = scores
                top = jnp.max(scores, axis=0, keepdims=True)
                high = top if high is None else jnp.maximum(high, top)
            sums = jnp.zeros_like(high)
            acc = jnp.zeros((HEAD_DIM, rows), F32)
            for c in range(KEY_PARTS):
                part = slice(c * chunk, (c + 1) * chunk)
                terms = jnp.exp(s_buf[part, :] - high)
                sums = sums + jnp.sum(terms, axis=0, keepdims=True)
                acc = acc + nn(v_t[h * HEAD_DIM : (h + 1) * HEAD_DIM, part], terms.astype(BF16))
            lse_out[h : h + 1, place] = high + jnp.log(sums)
            outs.append(acc / sums)
        o_t = jnp.concatenate(outs, axis=0)
        o_out[:, place] = o_t
        obuf[i] = o_t.T.astype(BF16)

        @pl.when(i > 0)
        def _():
            back_copy(i).start()

        return carry

    lax.fori_loop(0, n, block, 0)
    save = pltpu.make_async_copy(recv, heads, out_sem)
    save.start()
    land[:, own_lanes] = obuf[0]
    for i in range(1, n):
        for s in range(3):
            out_copy(s, i).wait_send()
        back_copy(i).wait_send()
        back_copy(i).wait_recv()
    att_out[...] = land[...]
    save.wait()


def backward_kernel(
    n, g_in, heads, o_t, lse, gh_out, gq_out, g_all, land, dk, dv, k_t,
    send, got, q_send, q_got, kv_send, kv_got,
):
    me = lax.axis_index("var")
    rows, dim = g_in.shape
    width = dim // n
    patches = rows * n
    mine = pl.ds(pl.multiple_of(me * rows, rows), rows)
    own_lanes = pl.ds(pl.multiple_of(me * width, width), width)
    greet(me, n)

    def out_copy(i):
        to = lax.rem(me + i, n)
        return pltpu.make_async_remote_copy(
            src_ref=g_in.at[:, pl.ds(pl.multiple_of(to * width, width), width)],
            dst_ref=g_all.at[mine, :],
            send_sem=send.at[i],
            recv_sem=got.at[i],
            device_id={"var": to},
            device_id_type=MESH,
        )

    def part_lanes(s):
        return pl.ds(pl.multiple_of(s * dim + me * width, width), width)

    def q_copy(i):
        to = lax.rem(me - i + n, n)
        return pltpu.make_async_remote_copy(
            src_ref=gh_out.at[0, pl.ds(pl.multiple_of(to * rows, rows), rows), :],
            dst_ref=land.at[:, part_lanes(0)],
            send_sem=q_send.at[i],
            recv_sem=q_got.at[i],
            device_id={"var": to},
            device_id_type=MESH,
        )

    def kv_copy(s, i):
        to = lax.rem(me + i, n)
        return pltpu.make_async_remote_copy(
            src_ref=gh_out.at[s, pl.ds(pl.multiple_of(to * rows, rows), rows), :],
            dst_ref=land.at[:, part_lanes(s)],
            send_sem=kv_send.at[s - 1, i],
            recv_sem=kv_got.at[s - 1, i],
            device_id={"var": to},
            device_id_type=MESH,
        )

    for i in range(1, n):
        out_copy(i).start()
    g_all[mine, :] = g_in[:, own_lanes]
    masks = head_masks(width)
    k_t[...] = heads[1].T
    dk[...] = jnp.zeros_like(dk)
    dv[...] = jnp.zeros_like(dv)
    chunk = patches // KEY_PARTS

    def block(i, carry):
        source = lax.rem(me - i + n, n)

        @pl.when(i > 0)
        def _():
            out_copy(i).wait_recv()

        place = pl.ds(pl.multiple_of(source * rows, rows), rows)
        q = heads[0, place, :].astype(F32) * FACTOR
        grad = g_all[place, :].astype(F32)
        products = grad.T * o_t[:, place]
        outs = []
        for h, mask in enumerate(masks):
            qh = (q * mask).astype(BF16)
            gh = (grad * mask).astype(BF16)
            span = slice(h * HEAD_DIM, (h + 1) * HEAD_DIM)
            rowdot = jnp.sum(products[span], axis=0, keepdims=True)
            total = lse[h : h + 1, place]
            acc = jnp.zeros((HEAD_DIM, rows), F32)
            for c in range(KEY_PARTS):
                part = slice(c * chunk, (c + 1) * chunk)
                probs = jnp.exp(nt(heads[1, part, :], qh) - total)
                g_probs = nt(heads[2, part, :], gh)
                g_scores = (probs * (g_probs - rowdot)).astype(BF16)
                dv[part, :] += nn(probs.astype(BF16), gh)
                dk[part, :] += nn(g_scores, qh)
                acc = acc + nn(k_t[span, part], g_scores)
            outs.append(acc * FACTOR)
        gh_out[0, place, :] = jnp.concatenate(outs, axis=0).T.astype(BF16)

        @pl.when(i > 0)
        def _():
            q_copy(i).start()

        return carry

    lax.fori_loop(0, n, block, 0)
    gh_out[1] = dk[...].astype(BF16)
    gh_out[2] = dv[...].astype(BF16)
    for i in range(1, n):
        for s in (1, 2):
            kv_copy(s, i).start()
    for s in range(3):
        land[:, part_lanes(s)] = gh_out[s, mine, :]
    for i in range(1, n):
        out_copy(i).wait_send()
        q_copy(i).wait_send()
        q_copy(i).wait_recv()
        for s in (1, 2):
            kv_copy(s, i).wait_send()
            kv_copy(s, i).wait_recv()
    gq_out[...] = land[...]


VMEM = pl.BlockSpec(memory_space=pltpu.VMEM)


def attention_forward_call(qkv, n):
    rows, total = qkv.shape
    dim = total // 3
    width = dim // n
    patches = rows * n
    sems = pltpu.SemaphoreType.DMA
    return pl.pallas_call(
        functools.partial(forward_kernel, n),
        out_shape=(
            jax.ShapeDtypeStruct((3, patches, width), BF16),
            jax.ShapeDtypeStruct((width, patches), F32),
            jax.ShapeDtypeStruct((width // HEAD_DIM, patches), F32),
            jax.ShapeDtypeStruct((rows, dim), BF16),
        ),
        in_specs=[VMEM],
        out_specs=(pl.BlockSpec(memory_space=pl.ANY), VMEM, VMEM, VMEM),
        scratch_shapes=[
            pltpu.VMEM((3, patches, width), BF16),
            pltpu.VMEM((rows, dim), BF16),
            pltpu.VMEM((n, rows, width), BF16),
            pltpu.VMEM((width, patches), BF16),
            pltpu.VMEM((patches, rows), F32),
            sems((3, n)),
            sems((3, n)),
            sems((n,)),
            sems((n,)),
            sems,
        ],
        compiler_params=pltpu.CompilerParams(collective_id=0, has_side_effects=True),
        cost_estimate=pl.CostEstimate(
            flops=40_000_000_000, bytes_accessed=8_000_000, transcendentals=0
        ),
        name="attention_forward",
    )(qkv)


def attention_backward_call(g_att, heads, o_t, lse, n):
    rows, dim = g_att.shape
    width = dim // n
    patches = rows * n
    sems = pltpu.SemaphoreType.DMA
    return pl.pallas_call(
        functools.partial(backward_kernel, n),
        out_shape=(
            jax.ShapeDtypeStruct((3, patches, width), BF16),
            jax.ShapeDtypeStruct((rows, 3 * dim), BF16),
        ),
        in_specs=[VMEM] * 4,
        out_specs=(VMEM, VMEM),
        scratch_shapes=[
            pltpu.VMEM((patches, width), BF16),
            pltpu.VMEM((rows, 3 * dim), BF16),
            pltpu.VMEM((patches, width), F32),
            pltpu.VMEM((patches, width), F32),
            pltpu.VMEM((width, patches), BF16),
            sems((n,)),
            sems((n,)),
            sems((n,)),
            sems((n,)),
            sems((2, n)),
            sems((2, n)),
        ],
        compiler_params=pltpu.CompilerParams(collective_id=1, has_side_effects=True),
        cost_estimate=pl.CostEstimate(
            flops=60_000_000_000, bytes_accessed=8_000_000, transcendentals=0
        ),
        name="attention_backward",
    )(g_att, heads, o_t, lse)


def body(
    pixels,
    dataset,
    var_mask,
    data_weight,
    emb_weight,
    var_embed,
    agg_query,
    agg_key,
    agg_value,
    agg_out,
    ln1_gain,
    ln1_bias,
    qkv_weight,
    proj_weight,
    ln2_gain,
    ln2_bias,
    fc1_weight,
    fc1_bias,
    fc2_weight,
    fc2_bias,
    cotangent,
):
    g = pixels.shape[0]
    slots = var_mask.shape[1]
    pix = pixels.shape[2]
    lanes = lax.axis_size("var")
    own_slots = slots // lanes
    mine = lax.axis_index("var")
    r = PATCHES // lanes
    rows = g * r
    live = slots // 4 * 3
    hot = (dataset[:, None] == jnp.arange(NDATA, dtype=jnp.int32)[None, :]).astype(F32)
    counts = data_weight.astype(F32)
    item_scale = jnp.dot(hot, counts, precision=PRECISE) * NDATA / jnp.sum(counts)
    mask = listed(jnp.dot(hot, var_mask.astype(F32), precision=PRECISE), 1)

    own_table = jnp.concatenate([emb_weight, var_embed[:, None, :]], axis=1)
    table = lax.all_gather(own_table, "var", axis=0, tiled=True)
    table = jnp.transpose(listed(table, 0), (1, 0, 2))
    flat_table = table.reshape((pix + 1) * live, D)
    patch_pix = lax.all_to_all(pixels, "var", split_axis=3, concat_axis=1, tiled=True)
    patch_pix = jnp.transpose(listed(patch_pix, 1), (0, 2, 1, 3))
    xs = jnp.concatenate([patch_pix, jnp.ones((g, 1, live, r), BF16)], axis=1)

    query_full = agg_query.astype(F32)
    key_full = agg_key.astype(F32)
    probe = (key_full * query_full[None, :]).reshape(D, HEADS, HEAD_DIM).sum(axis=-1)
    probe = probe.T.astype(BF16)
    seen = mm("xd,hd->hx", flat_table, probe).reshape(HEADS, pix + 1, live) * FACTOR
    ev = mm("xd,de->xe", flat_table, agg_value).astype(BF16)
    ev_heads = ev.reshape(pix + 1, live, HEADS, HEAD_DIM)

    xf = xs.astype(F32)
    scores = sum(seen[None, :, c, :, None] * xf[:, None, c] for c in range(pix + 1))
    present = mask[:, None, :, None]
    scores = jnp.where(present > 0.5, scores, -1e30)
    highest = jnp.max(scores, axis=2, keepdims=True)
    terms = jnp.exp(scores - highest) * present
    weights = terms / jnp.sum(terms, axis=2, keepdims=True)
    low = weights.astype(BF16)
    wx = low[:, :, None] * xs[:, None]
    mixed = mm("ghcvr,cvhe->grhe", wx, ev_heads).astype(BF16).reshape(rows, D)
    result = jnp.dot(mixed, agg_out, preferred_element_type=F32)

    vectors = [v.astype(F32) for v in (ln1_gain, ln1_bias, ln2_gain, ln2_bias, fc1_bias, fc2_bias)]
    gain1, shift1, gain2, shift2, bias1, bias2 = vectors
    normed1, inv1 = norm_stats(result)
    first = (normed1 * gain1 + shift1).astype(BF16)
    qkv = jnp.dot(first, qkv_weight, preferred_element_type=F32).astype(BF16).reshape(g, r, 3 * D)

    by_head = HEAD_DIM * HEADS == 128 * lanes and g == 1
    if by_head:
        heads, o_t, lse, attended = attention_forward_call(qkv[0], lanes)
    else:
        queries = qkv[..., :D].reshape(g, r, HEADS, HEAD_DIM)
        pair = lax.all_gather(qkv[..., D:], "var", axis=1, tiled=True)
        pair = pair.reshape(g, PATCHES, 2, HEADS, HEAD_DIM)
        keys, values = pair[:, :, 0], pair[:, :, 1]
        att_full, lse = attention_forward(queries, keys, values)
        attended = att_full.astype(BF16).reshape(rows, D)

    residual = result + jnp.dot(attended, proj_weight, preferred_element_type=F32)
    normed2, inv2 = norm_stats(residual)
    second = (normed2 * gain2 + shift2).astype(BF16)
    pre = jnp.dot(second, fc1_weight, preferred_element_type=F32) + bias1
    cdf = 0.5 * (1.0 + lax.erf(pre * (0.5**0.5)))
    slope = cdf + pre * jnp.exp(-0.5 * pre * pre) * 0.3989422804014327
    act = (pre * cdf).astype(BF16)
    block_out = residual + jnp.dot(act, fc2_weight, preferred_element_type=F32) + bias2

    g_final = (cotangent.astype(F32) * item_scale[:, None, None]).reshape(rows, D)
    g_mlp = g_final.astype(BF16)
    fc2_t = mm("rd,rf->df", g_mlp, act).astype(BF16)
    g_pre = (mm("rd,fd->rf", g_mlp, fc2_weight) * slope).astype(BF16)
    fc1_t = mm("rf,rd->fd", g_pre, second).astype(BF16)
    g_second = mm("rf,df->rd", g_pre, fc1_weight)
    g_resid = g_final + norm_back(g_second, gain2, normed2, inv2)
    g_branch = g_resid.astype(BF16)
    proj_t = mm("re,rd->ed", g_branch, attended).astype(BF16)
    g_att = mm("re,de->rd", g_branch, proj_weight).astype(BF16)
    if by_head:
        g_heads, g_qkv = attention_backward_call(g_att, heads, o_t, lse, lanes)
    else:
        g_att = g_att.reshape(att_full.shape)
        rowdot = jnp.sum(g_att.astype(F32) * att_full, axis=-1)
        rowdot = jnp.transpose(rowdot, (0, 2, 1))[..., None]
        g_q, g_k, g_v = attention_back(queries, keys, values, g_att, lse, rowdot)
        parts = [
            lax.psum_scatter(t, "var", scatter_dimension=1, tiled=True).reshape(g, r, D)
            for t in (g_k, g_v)
        ]
        g_qkv = jnp.concatenate([g_q.reshape(g, r, D)] + parts, axis=-1).astype(BF16)
    g_qkv = g_qkv.reshape(rows, 3 * D)
    qkv_t = mm("re,rd->ed", g_qkv, first).astype(BF16)
    g_first = mm("re,de->rd", g_qkv, qkv_weight)
    g_result = (g_resid + norm_back(g_first, gain1, normed1, inv1)).astype(BF16)
    out_t = mm("rd,rj->dj", g_result, mixed).astype(BF16)
    g_mixed = mm("rd,jd->rj", g_result, agg_out).astype(BF16).reshape(g, r, HEADS, HEAD_DIM)

    back = mm("cvhe,grhe->ghcvr", ev_heads, g_mixed)
    g_w = jnp.sum(back * xf[:, None], axis=2)
    rowsum = jnp.sum(weights * g_w, axis=2, keepdims=True)
    g_s = weights * (g_w - rowsum)
    pixel_grads = jnp.sum(low.astype(F32)[:, :, None] * back[:, :, :pix], axis=1)
    pixel_grads = pixel_grads + jnp.sum(
        g_s[:, :, None] * seen[None, :, :pix, :, None], axis=1
    )
    pixel_grads = unlisted(jnp.transpose(pixel_grads, (0, 2, 1, 3)).astype(BF16), 1)
    pixel_out = lax.all_to_all(pixel_grads, "var", split_axis=1, concat_axis=3, tiled=True)
    t_part = jnp.sum(g_s[:, :, None] * xf[:, None], axis=(0, 4))
    m_part = mm("ghcvr,grhe->cvhe", wx, g_mixed).reshape((pix + 1) * live, D)

    small = [
        jnp.sum(g_second * normed2, axis=0),
        jnp.sum(g_second, axis=0),
        jnp.sum(g_first * normed1, axis=0),
        jnp.sum(g_first, axis=0),
        jnp.sum(g_mlp.astype(F32), axis=0),
        jnp.sum(g_pre.astype(F32), axis=0),
        t_part.reshape(-1),
    ]
    sizes = [s.shape[0] for s in small]
    small_sum, m_sum = lax.psum((jnp.concatenate(small), m_part), ("item", "var"))
    ends = [sum(sizes[:k]) for k in range(len(sizes) + 1)]
    pieces = [small_sum[ends[k] : ends[k + 1]] for k in range(len(sizes))]

    def own(vector):
        width = vector.shape[0] // lanes
        return lax.dynamic_slice_in_dim(vector, mine * width, width)

    ln2_gain_grad, ln2_bias_grad, ln1_gain_grad, ln1_bias_grad, fc2_bias_grad, fc1_bias_grad = [
        own(p) for p in pieces[:6]
    ]
    t_sum = pieces[6].reshape(HEADS, (pix + 1) * live)

    m_slots = unlisted(m_sum.reshape(pix + 1, live, D), 1)
    t_slots = unlisted(t_sum.reshape(HEADS, pix + 1, live), 2)
    m_own = lax.dynamic_slice_in_dim(m_slots, mine * own_slots, own_slots, axis=1)
    t_own = lax.dynamic_slice_in_dim(t_slots, mine * own_slots, own_slots, axis=2)
    table_grad = mm("cve,de->vcd", m_own.astype(BF16), agg_value)
    table_grad = table_grad + jnp.einsum(
        "hcv,hd->vcd", t_own * FACTOR, probe.astype(F32), precision=PRECISE
    )
    width = D // lanes
    m_cols = lax.dynamic_slice_in_dim(m_sum, mine * width, width, axis=1)
    value_grad = mm("xd,xe->de", flat_table, m_cols.astype(BF16))
    g_probe = jnp.dot(t_sum, flat_table.astype(F32), precision=PRECISE) * FACTOR
    head_of = jnp.arange(D) // HEAD_DIM
    own_head = lax.dynamic_slice_in_dim(head_of, mine * width, width)
    pick = (own_head[None, :] == jnp.arange(HEADS)[:, None]).astype(F32)
    g_cols = jnp.einsum("hk,he->ke", g_probe, pick, precision=PRECISE)
    own_query = lax.dynamic_slice_in_dim(query_full, mine * width, width)
    own_key = lax.dynamic_slice_in_dim(agg_key, mine * width, width, axis=1).astype(F32)
    key_grad = g_cols * own_query[None, :]
    query_grad = jnp.sum(g_cols * own_key, axis=0)

    def reduced(grad):
        share = lax.psum_scatter(grad, "var", scatter_dimension=0, tiled=True)
        return lax.psum(share, "item").astype(F32).T

    fc2_grad, fc1_grad, proj_grad, qkv_grad, out_grad = [
        reduced(t) for t in (fc2_t, fc1_t, proj_t, qkv_t, out_t)
    ]
    return (
        block_out.reshape(g, r, D).astype(BF16),
        pixel_out,
        table_grad[:, :pix],
        table_grad[:, pix],
        query_grad,
        key_grad,
        value_grad,
        out_grad,
        ln1_gain_grad,
        ln1_bias_grad,
        qkv_grad,
        proj_grad,
        ln2_gain_grad,
        ln2_bias_grad,
        fc1_grad,
        fc1_bias_grad,
        fc2_grad,
        fc2_bias_grad,
    )


def solution(mesh):
    in_specs = (
        P("item", "var", None, None),
        P("item"),
        P(),
        P(),
        P("var", None, None),
        P("var", None),
        *([P()] * 14),
        P("item", "var", None),
    )
    cols = P(None, "var")
    vec = P("var")
    out_specs = (
        P("item", "var", None),
        P("item", "var", None, None),
        P("var", None, None),
        P("var", None),
        vec,
        cols,
        cols,
        cols,
        vec,
        vec,
        cols,
        cols,
        vec,
        vec,
        cols,
        vec,
        cols,
        vec,
    )
    return jax.shard_map(body, mesh=mesh, in_specs=in_specs, out_specs=out_specs, check_vma=False)
```
